32 devices in a mesh: shots: 2 (over x), gz: 8 (over z, y), gy: 2 (over core).
Axes of the slice: x: 2, y: 2, z: 4, core: 2. Of those that a mesh axis runs over, the one named last changes fastest.
Arguments:
- pressure: float32 [256, 64, 512], P(('shots', 'gz'), 'gy'), parts along dimension 0, may hold values from -6 to 6
- previous: float32 [256, 64, 512], P(('shots', 'gz'), 'gy'), parts along dimension 0, may hold values from -6 to 6
- memory: float32 [3, 256, 64, 512], P(None, ('shots', 'gz'), 'gy'), parts along dimension 1, may hold values from -6 to 6
- courant: float32 [128, 64, 512], P('gz', 'gy'), may hold values from 0.05 to 0.25
- quality: float32 [128, 64, 512], P('gz', 'gy'), may hold values from 0.05 to 0.3
- sponge: int32 [128, 64, 512], P('gz', 'gy'), may hold values from 0 to 1, as said below
- relax_time: float32 [3], replicated, may hold values from 2 to 40
- receiver_cell: int32 [8, 2048], P(None, ('gz', 'gy')), may hold values from 0 to 262143
- receiver_weight: float32 [8, 2048], P(None, ('gz', 'gy')), may hold values from 0 to 1
- output_order: int32 [2048], P(('gz', 'gy')), may hold values from 0 to 2047, each once
Outputs:
- traces: float32 [48, 2048], P('shots', ('gz', 'gy')), parts along dimension 0
- pressure_out: float32 [256, 64, 512], P(('shots', 'gz'), 'gy'), parts along dimension 0
The draws below stay inside these ranges and needn't reach their ends.
There are 2 independent parts, one for each index of `shots`. The reference program is written for one: setup_inputs(seed, part) draws one part's arguments, and reference() takes and returns one part's arrays. A program takes and returns all parts, laid end to end along the dimension named above; an argument that names none is the same for every part. Nothing has to cross between parts.
Inputs may be any that keep to these rules, and one draw needn't show every extreme that they name: sponge is 1 exactly in the first and last few inline cells, possibly the first and last few crossline cells and the deepest cells of the grid. `output_order`: each receiver appears once.
All inputs are finite; a program needn't handle non-finite values.
Results may differ from the reference program's by a relative error of at most 0.0001.
Values sent between devices are 32-bit elements; how exact they have to be, the bound alone decides.
A program may use at most 64 MiB of HBM per device.

```python
import math
import jax
import jax.numpy as jnp
from jax import lax

CZ = 16
CY = 32
NX = 512
REC_DEV = 128
MECH = 3
CORNERS = 8
NZ = 128
NY = 64
RECS = 2048
TIME = 24
N_GY = 2


def draw_sponge(key, part):
    near_width = jax.random.randint(jax.random.fold_in(key, 11), (), NX // 16, NX // 8 + 1)
    far_width = jax.random.randint(jax.random.fold_in(key, 12), (), NX // 16, NX // 8 + 1)
    side_width = jax.random.randint(jax.random.fold_in(key, 13), (), 0, NY // 8 + 1)
    bottom_width = jax.random.randint(jax.random.fold_in(key, 14), (), NZ // 8, NZ // 4 + 1)
    depth_index = lax.broadcasted_iota(jnp.int32, (NZ, NY, NX), 0)
    cross_index = lax.broadcasted_iota(jnp.int32, (NZ, NY, NX), 1)
    inline_index = lax.broadcasted_iota(jnp.int32, (NZ, NY, NX), 2)
    inside = (inline_index < near_width) | (inline_index >= NX - far_width)
    inside = inside | (cross_index < side_width) | (cross_index >= NY - side_width)
    inside = inside | (depth_index >= NZ - bottom_width)
    return jnp.where(inside, 1, 0).astype(jnp.int32)


def place_ends(result, rng, smallest, top_value):
    extent = result.shape
    spot = [jax.random.randint(jax.random.fold_in(rng, axis), (), 0, extent[axis]) for axis in range(len(extent))]
    result = result.at[tuple(spot)].set(smallest)
    longest = extent.index(max(extent))
    spot[longest] = (spot[longest] + 1) % extent[longest]
    return result.at[tuple(spot)].set(top_value)


def steps_of(rng, shape, shards, low, high):
    loudness = 1.0
    for position, shards_of in shards:
        draws = jax.random.uniform(jax.random.fold_in(jax.random.fold_in(rng, 6), position), (shards_of,), jnp.float32, low / len(shards), high / len(shards))
        loudness = loudness * jnp.repeat(jnp.exp(draws), shape[position] // shards_of).reshape((-1,) + (1,) * (len(shape) - 1 - position))
    return loudness


def centred(key, shape, scale, limit, pieces=(), kind=jnp.bfloat16):
    drawn = jax.random.normal(key, shape, jnp.float32) * scale
    if len(pieces) > 0:
        drawn = steps_of(key, shape, pieces, -0.22, 0.18) * drawn
    return jnp.clip(drawn, min=-limit, max=limit).astype(kind)


def setup_inputs(seed: int = 0, part: int = 0) -> dict:
    streams_of = jax.random.split(jax.random.key(seed), 11)
    part_splits = jax.random.split(jax.random.fold_in(streams_of[10], part), 11)
    pressure = centred(part_splits[0], (NZ, NY, NX), 1.0, 6.0, ((0, 8), (1, 2)), jnp.float32)
    previous = centred(part_splits[1], (NZ, NY, NX), 1.0, 6.0, ((0, 8), (1, 2)), jnp.float32)
    memory = centred(part_splits[2], (MECH, NZ, NY, NX), 1.0, 6.0, ((1, 8), (2, 2)), jnp.float32)
    courant = jnp.clip(0.05 + 0.2 * jax.random.uniform(streams_of[3], (NZ, NY, NX), jnp.float32) ** steps_of(streams_of[3], (NZ, NY, NX), ((0, 8), (1, 2)), -0.2, 0.2), 0.05, 0.25)
    quality = jnp.clip(0.05 + 0.25 * jax.random.uniform(streams_of[4], (NZ, NY, NX), jnp.float32) ** steps_of(streams_of[4], (NZ, NY, NX), ((0, 8), (1, 2)), -0.2, 0.2), 0.05, 0.3)
    sponge = draw_sponge(jax.random.fold_in(streams_of[10], 71), part)
    relax_time = jnp.clip(jnp.exp(jax.random.uniform(streams_of[6], (MECH,), jnp.float32, math.log(2.0), math.log(40.0))), 2.0, 40.0)
    receiver_cell = place_ends(jax.random.randint(streams_of[7], (CORNERS, RECS), 0, CZ * CY * NX), jax.random.fold_in(streams_of[7], 1), 0, (CZ * CY * NX) - 1).astype(jnp.int32)
    receiver_weight = jnp.clip(1.0 * jax.random.uniform(streams_of[8], (CORNERS, RECS), jnp.float32) ** steps_of(streams_of[8], (CORNERS, RECS), ((1, 16),), -0.2, 0.2), 0.0, 1.0)
    output_order = jax.random.permutation(streams_of[9], RECS).astype(jnp.int32)
    return {"pressure": pressure, "previous": previous, "memory": memory, "courant": courant, "quality": quality, "sponge": sponge, "relax_time": relax_time, "receiver_cell": receiver_cell, "receiver_weight": receiver_weight, "output_order": output_order}


sponge_rate = 0.2


def laplace(padded):
    middle = padded[1:-1, 1:-1, :]
    sides = jnp.pad(middle, ((0, 0), (0, 0), (1, 1)))
    summed = padded[2:, 1:-1, :] + padded[:-2, 1:-1, :]
    summed = summed + padded[1:-1, 2:, :] + padded[1:-1, :-2, :]
    summed = summed + sides[:, :, 2:] + sides[:, :, :-2]
    return summed - 6.0 * middle


def advance(padded, earlier, memory, courant, quality, damping, decays):
    stencil = laplace(padded)
    middle = padded[1:-1, 1:-1, :]
    retain = decays[:, None, None, None]
    memory = retain * memory + (1.0 - retain) * stencil[None]
    forcing = stencil + quality * (stencil - jnp.mean(memory, axis=0))
    updated = (2.0 * middle - (1.0 - damping) * earlier + courant * forcing) / (1.0 + damping)
    return updated, memory


def reference(pressure, previous, memory, courant, quality, sponge, relax_time, receiver_cell, receiver_weight, output_order):
    damping = sponge_rate * sponge.astype(jnp.float32)
    decays = jnp.exp(-1.0 / relax_time)
    receiver = jnp.arange(RECS, dtype=jnp.int32)
    owner_device = receiver // REC_DEV
    slab_index = owner_device // N_GY
    cross_index = owner_device % N_GY
    local_depth = receiver_cell // (CY * NX)
    local_cross = (receiver_cell // NX) % CY
    local_inline = receiver_cell % NX
    global_cell = ((slab_index[None, :] * CZ + local_depth) * NY + cross_index[None, :] * CY + local_cross) * NX + local_inline
    global_cell = global_cell.astype(jnp.int32)

    def one_step(carried, unused):
        current, earlier, mem_state = carried
        padded = jnp.pad(current, ((1, 1), (1, 1), (0, 0)))
        updated, mem_state = advance(padded, earlier, mem_state, courant, quality, damping, decays)
        picked = jnp.take(updated.reshape(-1), global_cell, axis=0)
        return (updated, current, mem_state), jnp.sum(picked * receiver_weight, axis=0)

    carried, samples = lax.scan(one_step, (pressure, previous, memory), None, length=TIME)
    traces = jnp.take(samples, output_order, axis=1)
    return traces, carried[0]
```

```python
import jax
import jax.numpy as jnp
from jax import lax
from jax.experimental import pallas as pl
from jax.experimental.pallas import tpu as pltpu
from jax.sharding import PartitionSpec as P

TIME = 24
MECH = 3
SPONGE_RATE = 0.2
SUB = 8
LANE = 128
MESH = pl.DeviceIdType.MESH


def to_rows(block):
    y, x = block.shape[-2:]
    lead = block.size // (y * x)
    tiles = block.reshape(lead, y // SUB, SUB, x // LANE, LANE)
    return tiles.transpose(0, 1, 3, 2, 4).reshape(block.size // LANE, LANE)


def from_rows(rows, shape):
    z, y, x = shape
    tiles = rows.reshape(z, y // SUB, x // LANE, SUB, LANE)
    return tiles.transpose(0, 1, 3, 2, 4).reshape(shape)


def make_kernel(cz, cy, nx, n_gz, n_gy, corners, recs):
    yt, xt = cy // SUB, nx // LANE
    plane = cy * nx // LANE
    block = cz * plane
    slot = (cz + 2) * plane + SUB
    slots = TIME + 2

    def kernel(
        pressure, previous, memory, courant, quality, sponge, decays, rows, lanes, weights,
        samples, pressure_out,
        hist, mem, ca, cb, sp, inv2, ysend, yrecv,
        load_sem, zsend_sem, zrecv_sem, ysend_sem, yrecv_sem, out_sem,
    ):
        gz = lax.axis_index("gz")
        gy = lax.axis_index("gy")
        z_has = (gz > 0, gz < n_gz - 1)
        y_has = (gy > 0, gy < n_gy - 1)
        z_dev = (jnp.maximum(gz - 1, 0), jnp.minimum(gz + 1, n_gz - 1))
        y_dev = (jnp.maximum(gy - 1, 0), jnp.minimum(gy + 1, n_gy - 1))

        def hist_at(level, p):
            return pl.multiple_of(level * slot + p * plane, SUB)

        loads = [
            pltpu.make_async_copy(pressure, hist.at[pl.ds(slot + plane, block)], load_sem.at[0]),
            pltpu.make_async_copy(courant, ca, load_sem.at[1]),
            pltpu.make_async_copy(quality, cb, load_sem.at[2]),
            pltpu.make_async_copy(sponge, sp, load_sem.at[3]),
            pltpu.make_async_copy(previous, hist.at[pl.ds(plane, block)], load_sem.at[4]),
            pltpu.make_async_copy(memory, mem, load_sem.at[5]),
        ]
        for copy in loads:
            copy.start()

        barrier = pltpu.get_barrier_semaphore()
        for side in range(2):
            @pl.when(z_has[side])
            def _():
                pl.semaphore_signal(barrier, inc=1, device_id={"gz": z_dev[side]}, device_id_type=MESH)

            @pl.when(y_has[side])
            def _():
                pl.semaphore_signal(barrier, inc=1, device_id={"gy": y_dev[side]}, device_id_type=MESH)

        zero = jnp.zeros((SUB, LANE), jnp.float32)
        for side in range(2):
            @pl.when(jnp.logical_not(z_has[side]))
            def _():
                def fill(level, carry):
                    base = hist_at(level, side * (cz + 1))
                    for i in range(plane // SUB):
                        hist[pl.ds(base + i * SUB, SUB), :] = zero
                    return carry
                lax.fori_loop(1, slots, fill, 0)

            @pl.when(jnp.logical_not(y_has[side]))
            def _():
                def fill(level, carry):
                    for q in range(cz):
                        yrecv[level, side, q] = jnp.zeros((xt, LANE), jnp.float32)
                    return carry
                lax.fori_loop(1, slots, fill, 0)

        peers = sum(has.astype(jnp.int32) for has in z_has + y_has)
        pl.semaphore_wait(barrier, peers)

        part = xt * SUB

        def z_copy(level, side, chunk):
            source = hist_at(level, (1, cz)[side]) + chunk * part
            target = hist_at(level, (cz + 1, 0)[side]) + chunk * part
            par = level % 2
            return pltpu.make_async_remote_copy(
                src_ref=hist.at[pl.ds(pl.multiple_of(source, SUB), part)],
                dst_ref=hist.at[pl.ds(pl.multiple_of(target, SUB), part)],
                send_sem=zsend_sem.at[par, side, chunk],
                recv_sem=zrecv_sem.at[par, side, chunk],
                device_id={"gz": z_dev[side]},
                device_id_type=MESH,
            )

        def y_copy(level, side, piece):
            start, count = ((0, 2), (2, cz - 2))[piece]
            par = level % 2
            return pltpu.make_async_remote_copy(
                src_ref=ysend.at[level, side, pl.ds(start, count)],
                dst_ref=yrecv.at[level, 1 - side, pl.ds(start, count)],
                send_sem=ysend_sem.at[par, side, piece],
                recv_sem=yrecv_sem.at[par, side, piece],
                device_id={"gy": y_dev[side]},
                device_id_type=MESH,
            )

        def send(copy_of, has, level, index, go=None):
            for side in range(2):
                @pl.when(has[side] if go is None else has[side] & go)
                def _():
                    copy_of(level, side, index).start()

        def settle(copy_of, has, level, index):
            for side in range(2):
                @pl.when(has[side])
                def _():
                    copy_of(level, side, index).wait_send()
                    copy_of(level, 1 - side, index).wait_recv()

        def keep_rows(level, q, b, x, tile):
            if b == 0:
                ysend[level, 0, q, x:x + 1, :] = tile[0:1, :]
            if b == yt - 1:
                ysend[level, 1, q, x:x + 1, :] = tile[SUB - 1:SUB, :]

        loads[0].wait()
        for chunk in range(yt):
            send(z_copy, z_has, 1, chunk)

        def first_rows(z, q):
            base = hist_at(1, z + 1)
            for b in sorted({0, yt - 1}):
                for x in range(xt):
                    keep_rows(1, q, b, x, hist[pl.ds(base + (b * xt + x) * SUB, SUB), :])

        first_rows(0, 0)
        first_rows(cz - 1, 1)
        send(y_copy, y_has, 1, 0)

        def first_loop(z, carry):
            first_rows(z, z + 1)
            return carry
        lax.fori_loop(1, cz - 1, first_loop, 0)
        send(y_copy, y_has, 1, 1)

        for copy in loads[1:4]:
            copy.wait()

        def coefficients(i, carry):
            for j in range(4):
                at = pl.ds(pl.multiple_of((i * 4 + j) * SUB, SUB), SUB)
                two = 2.0 / (1.0 + SPONGE_RATE * sp[at, :].astype(jnp.float32))
                scaled = ca[at, :] * (0.5 * two)
                attenuation = cb[at, :]
                inv2[at, :] = two
                ca[at, :] = scaled * (1.0 + attenuation)
                cb[at, :] = scaled * attenuation * (1.0 / MECH)
            return carry
        lax.fori_loop(0, block // (4 * SUB), coefficients, 0)
        for copy in loads[4:]:
            copy.wait()

        lane = lax.broadcasted_iota(jnp.int32, (SUB, LANE), 1)
        sub = lax.broadcasted_iota(jnp.int32, (SUB, LANE), 0)
        lane_first, lane_last = lane == 0, lane == LANE - 1
        sub_first, sub_last = sub == 0, sub == SUB - 1
        retain = [decays[m] for m in range(MECH)]
        renew = [1.0 - r for r in retain]

        def advance(t, z, q, bands):
            now = hist_at(t + 1, z + 1)
            before = hist_at(t, z + 1)
            after = hist_at(t + 2, z + 1)
            cell = pl.multiple_of(z * plane, SUB)

            def tile_of(ref, base, b, x):
                return ref[pl.ds(pl.multiple_of(base + (b * xt + x) * SUB, SUB), SUB), :]

            for b in bands:
                mids = [tile_of(hist, now, b, x) for x in range(xt)]
                right = [pltpu.roll(v, 1, 1) for v in mids]
                left = [pltpu.roll(v, LANE - 1, 1) for v in mids]
                for x in range(xt):
                    c = mids[x]
                    xm = jnp.where(lane_first, right[x - 1] if x > 0 else 0.0, right[x])
                    xp = jnp.where(lane_last, left[x + 1] if x < xt - 1 else 0.0, left[x])
                    if b > 0:
                        edge = pltpu.roll(tile_of(hist, now, b - 1, x), 1, 0)
                    else:
                        edge = jnp.broadcast_to(yrecv[t + 1, 0, q, x:x + 1, :], (SUB, LANE))
                    ym = jnp.where(sub_first, edge, pltpu.roll(c, 1, 0))
                    if b < yt - 1:
                        edge = pltpu.roll(tile_of(hist, now, b + 1, x), SUB - 1, 0)
                    else:
                        edge = jnp.broadcast_to(yrecv[t + 1, 1, q, x:x + 1, :], (SUB, LANE))
                    yp = jnp.where(sub_last, edge, pltpu.roll(c, SUB - 1, 0))
                    zm = tile_of(hist, now - plane, b, x)
                    zp = tile_of(hist, now + plane, b, x)
                    s = ((zp + zm) + (yp + ym)) + (xp + xm) - 6.0 * c
                    total = None
                    for m in range(MECH):
                        at = pl.ds(pl.multiple_of(m * block + cell + (b * xt + x) * SUB, SUB), SUB)
                        value = retain[m] * mem[at, :] + renew[m] * s
                        mem[at, :] = value
                        total = value if total is None else total + value
                    e = tile_of(hist, before, b, x)
                    u = (e + tile_of(inv2, cell, b, x) * (c - e)) + (
                        tile_of(ca, cell, b, x) * s - tile_of(cb, cell, b, x) * total
                    )
                    hist[pl.ds(pl.multiple_of(after + (b * xt + x) * SUB, SUB), SUB), :] = u
                    keep_rows(t + 2, q, b, x, u)

        def step(t, carry):
            go = t < TIME - 1
            settle(y_copy, y_has, t + 1, 0)
            for b in range(yt):
                settle(z_copy, z_has, t + 1, b)
                advance(t, 0, 0, [b])
                advance(t, cz - 1, 1, [b])
                send(z_copy, z_has, t + 2, b, go)
            send(y_copy, y_has, t + 2, 0, go)
            settle(y_copy, y_has, t + 1, 1)

            def inner(z, c):
                advance(t, z, z + 1, list(range(yt)))
                return c
            lax.fori_loop(1, cz - 1, inner, 0)
            send(y_copy, y_has, t + 2, 1, go)
            return carry
        lax.fori_loop(0, TIME, step, 0)

        result = pltpu.make_async_copy(
            hist.at[pl.ds((TIME + 1) * slot + plane, block)], pressure_out, out_sem)
        result.start()

        groups = TIME // SUB

        def record(r, found):
            sums = [jnp.zeros((SUB, LANE), jnp.float32) for _ in range(groups)]
            for c in range(corners):
                row = rows[c * recs + r]
                mask = jnp.where(lane == lanes[c * recs + r], weights[c * recs + r], 0.0)
                for g in range(groups):
                    start = (2 + g * SUB) * slot + plane + row
                    sums[g] = sums[g] + mask * hist[pl.ds(start, SUB, stride=slot), :]
            return tuple(
                jnp.where(lane == r, jnp.sum(sums[g], axis=1, keepdims=True), found[g])
                for g in range(groups))
        found = lax.fori_loop(
            0, recs, record,
            tuple(jnp.zeros((SUB, LANE), jnp.float32) for _ in range(groups)), unroll=4)
        for g in range(groups):
            samples[pl.ds(g * SUB, SUB), :] = found[g]
        result.wait()

    f32 = jnp.float32
    any_spec = pl.BlockSpec(memory_space=pl.ANY)
    smem = pl.BlockSpec(memory_space=pltpu.SMEM)
    return pl.pallas_call(
        kernel,
        out_shape=(
            jax.ShapeDtypeStruct((TIME, recs), f32),
            jax.ShapeDtypeStruct((block, LANE), f32),
        ),
        in_specs=[any_spec] * 6 + [smem] * 4,
        out_specs=(pl.BlockSpec(memory_space=pltpu.VMEM), any_spec),
        scratch_shapes=[
            pltpu.VMEM((slots * slot, LANE), f32),
            pltpu.VMEM((MECH * block, LANE), f32),
            pltpu.VMEM((block, LANE), f32),
            pltpu.VMEM((block, LANE), f32),
            pltpu.VMEM((block, LANE), jnp.int32),
            pltpu.VMEM((block, LANE), f32),
            pltpu.VMEM((slots, 2, cz, xt, LANE), f32),
            pltpu.VMEM((slots, 2, cz, xt, LANE), f32),
            pltpu.SemaphoreType.DMA((6,)),
            pltpu.SemaphoreType.DMA((2, 2, yt)),
            pltpu.SemaphoreType.DMA((2, 2, yt)),
            pltpu.SemaphoreType.DMA((2, 2, 2)),
            pltpu.SemaphoreType.DMA((2, 2, 2)),
            pltpu.SemaphoreType.DMA,
        ],
        compiler_params=pltpu.CompilerParams(
            collective_id=0, has_side_effects=True, vmem_limit_bytes=60 * 1024 * 1024,
        ),
    )


def solution(mesh):
    n_gz, n_gy = mesh.shape["gz"], mesh.shape["gy"]

    def on_device(
        pressure, previous, memory, courant, quality, sponge, relax_time,
        receiver_cell, receiver_weight, output_order,
    ):
        cz, cy, nx = pressure.shape
        corners, recs = receiver_cell.shape
        decays = jnp.exp(-1.0 / relax_time)
        x = receiver_cell % nx
        y = (receiver_cell // nx) % cy
        z = receiver_cell // (nx * cy)
        rows = ((z * (cy // SUB) + y // SUB) * (nx // LANE) + x // LANE) * SUB + y % SUB
        run = make_kernel(cz, cy, nx, n_gz, n_gy, corners, recs)
        samples, out = run(
            to_rows(pressure), to_rows(previous), to_rows(memory), to_rows(courant),
            to_rows(quality), to_rows(sponge), decays,
            rows.reshape(-1), (x % LANE).reshape(-1), receiver_weight.reshape(-1),
        )
        collected = lax.all_gather(samples, ("gz", "gy"), axis=1, tiled=True)
        pick = lax.broadcasted_iota(jnp.int32, (collected.shape[1], recs), 0) == output_order[None, :]
        traces = jnp.dot(collected, pick.astype(jnp.float32), precision=lax.Precision.HIGHEST)
        return traces, from_rows(out, (cz, cy, nx))

    in_specs = (
        P(("shots", "gz"), "gy", None),
        P(("shots", "gz"), "gy", None),
        P(None, ("shots", "gz"), "gy", None),
        P("gz", "gy", None),
        P("gz", "gy", None),
        P("gz", "gy", None),
        P(),
        P(None, ("gz", "gy")),
        P(None, ("gz", "gy")),
        P(("gz", "gy")),
    )
    out_specs = (P("shots", ("gz", "gy")), P(("shots", "gz"), "gy", None))
    return jax.shard_map(
        on_device, mesh=mesh, in_specs=in_specs, out_specs=out_specs, check_vma=False
    )
```

```python
import jax
import jax.numpy as jnp
from jax import lax
from jax.experimental import pallas as pl
from jax.experimental.pallas import tpu as pltpu
from jax.sharding import PartitionSpec as P

TIME = 24
MECH = 3
SPONGE_RATE = 0.2
SUB = 8
LANE = 128
MESH = pl.DeviceIdType.MESH


def to_rows(block):
    y, x = block.shape[-2:]
    lead = block.size // (y * x)
    tiles = block.reshape(lead, y // SUB, SUB, x // LANE, LANE)
    return tiles.transpose(0, 1, 3, 2, 4).reshape(block.size // LANE, LANE)


def from_rows(rows, shape):
    z, y, x = shape
    tiles = rows.reshape(z, y // SUB, x // LANE, SUB, LANE)
    return tiles.transpose(0, 1, 3, 2, 4).reshape(shape)


def make_kernel(cz, cy, nx, n_gz, n_gy, corners, recs):
    yt, xt = cy // SUB, nx // LANE
    plane = cy * nx // LANE
    block = cz * plane
    slot = block + SUB
    n_dev = n_gz * n_gy
    slots = TIME + 2

    def kernel(
        pressure, previous, memory, courant, quality, sponge, relax, rows, lanes, weights, order,
        traces, pressure_out,
        hist, zrecv, mem, ca, cb, sp, inv2, ysend, yrecv, samples, gathered, onehot,
        load_sem, zsend_sem, zrecv_sem, ysend_sem, yrecv_sem, gsend_sem, grecv_sem, out_sem,
    ):
        gz = lax.axis_index("gz")
        gy = lax.axis_index("gy")
        z_has = (gz > 0, gz < n_gz - 1)
        y_has = (gy > 0, gy < n_gy - 1)
        z_dev = (jnp.maximum(gz - 1, 0), jnp.minimum(gz + 1, n_gz - 1))
        y_dev = (jnp.maximum(gy - 1, 0), jnp.minimum(gy + 1, n_gy - 1))

        me = gz * n_gy + gy

        def device(index):
            return {"gz": index // n_gy, "gy": index % n_gy}

        def hist_at(level, p):
            return pl.multiple_of(level * slot + p * plane, SUB)

        def halo_at(level, side):
            return pl.multiple_of((level * 2 + side) * plane, SUB)

        loads = [
            pltpu.make_async_copy(pressure, hist.at[pl.ds(slot, block)], load_sem.at[0]),
            pltpu.make_async_copy(courant, ca, load_sem.at[1]),
            pltpu.make_async_copy(quality, cb, load_sem.at[2]),
            pltpu.make_async_copy(sponge, sp, load_sem.at[3]),
            pltpu.make_async_copy(previous, hist.at[pl.ds(0, block)], load_sem.at[4]),
            pltpu.make_async_copy(memory, mem, load_sem.at[5]),
        ]
        for copy in loads:
            copy.start()

        barrier = pltpu.get_barrier_semaphore()
        def greet(k, carry):
            pl.semaphore_signal(
                barrier, inc=1, device_id=device((me + k) % n_dev), device_id_type=MESH)
            return carry
        lax.fori_loop(1, n_dev, greet, 0)

        zero = jnp.zeros((SUB, LANE), jnp.float32)
        for side in range(2):
            @pl.when(jnp.logical_not(z_has[side]))
            def _():
                def fill(level, carry):
                    base = halo_at(level, side)
                    for i in range(plane // SUB):
                        zrecv[pl.ds(base + i * SUB, SUB), :] = zero
                    return carry
                lax.fori_loop(1, slots, fill, 0)

            @pl.when(jnp.logical_not(y_has[side]))
            def _():
                def fill(level, carry):
                    for q in range(cz):
                        yrecv[level, side, q] = jnp.zeros((xt, LANE), jnp.float32)
                    return carry
                lax.fori_loop(1, slots, fill, 0)

        pl.semaphore_wait(barrier, n_dev - 1)

        part = xt * SUB

        def z_copy(level, side, chunk):
            source = hist_at(level, (0, cz - 1)[side]) + chunk * part
            target = halo_at(level, 1 - side) + chunk * part
            par = level % 2
            return pltpu.make_async_remote_copy(
                src_ref=hist.at[pl.ds(pl.multiple_of(source, SUB), part)],
                dst_ref=zrecv.at[pl.ds(pl.multiple_of(target, SUB), part)],
                send_sem=zsend_sem.at[par, side, chunk],
                recv_sem=zrecv_sem.at[par, side, chunk],
                device_id={"gz": z_dev[side]},
                device_id_type=MESH,
            )

        def y_copy(level, side, piece):
            start, count = ((0, 2), (2, cz - 2))[piece]
            par = level % 2
            return pltpu.make_async_remote_copy(
                src_ref=ysend.at[level, side, pl.ds(start, count)],
                dst_ref=yrecv.at[level, 1 - side, pl.ds(start, count)],
                send_sem=ysend_sem.at[par, side, piece],
                recv_sem=yrecv_sem.at[par, side, piece],
                device_id={"gy": y_dev[side]},
                device_id_type=MESH,
            )

        def send(copy_of, has, level, index, go=None):
            for side in range(2):
                @pl.when(has[side] if go is None else has[side] & go)
                def _():
                    copy_of(level, side, index).start()

        def settle(copy_of, has, level, index):
            for side in range(2):
                @pl.when(has[side])
                def _():
                    copy_of(level, side, index).wait_send()
                    copy_of(level, 1 - side, index).wait_recv()

        def keep_rows(level, q, b, x, tile):
            if b == 0:
                ysend[level, 0, q, x:x + 1, :] = tile[0:1, :]
            if b == yt - 1:
                ysend[level, 1, q, x:x + 1, :] = tile[SUB - 1:SUB, :]

        loads[0].wait()
        for chunk in range(yt):
            send(z_copy, z_has, 1, chunk)

        def first_rows(z, q):
            base = hist_at(1, z)
            for b in sorted({0, yt - 1}):
                for x in range(xt):
                    keep_rows(1, q, b, x, hist[pl.ds(base + (b * xt + x) * SUB, SUB), :])

        first_rows(0, 0)
        first_rows(cz - 1, 1)
        send(y_copy, y_has, 1, 0)

        def first_loop(z, carry):
            first_rows(z, z + 1)
            return carry
        lax.fori_loop(1, cz - 1, first_loop, 0)
        send(y_copy, y_has, 1, 1)

        for copy in loads[1:4]:
            copy.wait()

        def coefficients(i, carry):
            for j in range(4):
                at = pl.ds(pl.multiple_of((i * 4 + j) * SUB, SUB), SUB)
                two = 2.0 / (1.0 + SPONGE_RATE * sp[at, :].astype(jnp.float32))
                scaled = ca[at, :] * (0.5 * two)
                attenuation = cb[at, :]
                inv2[at, :] = two
                ca[at, :] = scaled * (1.0 + attenuation)
                cb[at, :] = scaled * attenuation * (1.0 / MECH)
            return carry
        lax.fori_loop(0, block // (4 * SUB), coefficients, 0)
        for copy in loads[4:]:
            copy.wait()

        lane = lax.broadcasted_iota(jnp.int32, (SUB, LANE), 1)
        sub = lax.broadcasted_iota(jnp.int32, (SUB, LANE), 0)
        lane_first, lane_last = lane == 0, lane == LANE - 1
        sub_first, sub_last = sub == 0, sub == SUB - 1
        retain = [jnp.exp(-1.0 / jnp.full((SUB, LANE), relax[m], jnp.float32)) for m in range(MECH)]
        renew = [1.0 - r for r in retain]

        def advance(t, z, q, bands):
            now = hist_at(t + 1, z)
            before = hist_at(t, z)
            after = hist_at(t + 2, z)
            cell = pl.multiple_of(z * plane, SUB)
            first = isinstance(z, int) and z == 0
            last = isinstance(z, int) and z == cz - 1
            below = (zrecv, halo_at(t + 1, 0)) if first else (hist, now - plane)
            above = (zrecv, halo_at(t + 1, 1)) if last else (hist, now + plane)

            def tile_of(ref, base, b, x):
                return ref[pl.ds(pl.multiple_of(base + (b * xt + x) * SUB, SUB), SUB), :]

            for b in bands:
                mids = [tile_of(hist, now, b, x) for x in range(xt)]
                right = [pltpu.roll(v, 1, 1) for v in mids]
                left = [pltpu.roll(v, LANE - 1, 1) for v in mids]
                for x in range(xt):
                    c = mids[x]
                    xm = jnp.where(lane_first, right[x - 1] if x > 0 else 0.0, right[x])
                    xp = jnp.where(lane_last, left[x + 1] if x < xt - 1 else 0.0, left[x])
                    if b > 0:
                        edge = pltpu.roll(tile_of(hist, now, b - 1, x), 1, 0)
                    else:
                        edge = jnp.broadcast_to(yrecv[t + 1, 0, q, x:x + 1, :], (SUB, LANE))
                    ym = jnp.where(sub_first, edge, pltpu.roll(c, 1, 0))
                    if b < yt - 1:
                        edge = pltpu.roll(tile_of(hist, now, b + 1, x), SUB - 1, 0)
                    else:
                        edge = jnp.broadcast_to(yrecv[t + 1, 1, q, x:x + 1, :], (SUB, LANE))
                    yp = jnp.where(sub_last, edge, pltpu.roll(c, SUB - 1, 0))
                    zm = tile_of(*below, b, x)
                    zp = tile_of(*above, b, x)
                    s = ((zp + zm) + (yp + ym)) + (xp + xm) - 6.0 * c
                    total = None
                    for m in range(MECH):
                        at = pl.ds(pl.multiple_of(m * block + cell + (b * xt + x) * SUB, SUB), SUB)
                        value = retain[m] * mem[at, :] + renew[m] * s
                        mem[at, :] = value
                        total = value if total is None else total + value
                    e = tile_of(hist, before, b, x)
                    u = (e + tile_of(inv2, cell, b, x) * (c - e)) + (
                        tile_of(ca, cell, b, x) * s - tile_of(cb, cell, b, x) * total
                    )
                    hist[pl.ds(pl.multiple_of(after + (b * xt + x) * SUB, SUB), SUB), :] = u
                    keep_rows(t + 2, q, b, x, u)

        def step(t, carry):
            go = t < TIME - 1
            settle(y_copy, y_has, t + 1, 0)
            for b in range(yt):
                settle(z_copy, z_has, t + 1, b)
                advance(t, 0, 0, [b])
                advance(t, cz - 1, 1, [b])
                send(z_copy, z_has, t + 2, b, go)
            send(y_copy, y_has, t + 2, 0, go)
            settle(y_copy, y_has, t + 1, 1)

            def inner(z, c):
                advance(t, z, z + 1, list(range(yt)))
                return c
            lax.fori_loop(1, cz - 1, inner, 0)
            send(y_copy, y_has, t + 2, 1, go)

            @pl.when(t >= SUB)
            def _():
                found_at(t // SUB - 1, (t % SUB) * share, share, 4)
            return carry

        groups = TIME // SUB
        share = recs // SUB

        def found_at(g, begin, count, unroll):
            at = pl.ds(pl.multiple_of(g * SUB, SUB), SUB)
            level = (2 + g * SUB) * slot

            def record(i, found):
                r = begin + i
                sums = jnp.zeros((SUB, LANE), jnp.float32)
                for c in range(corners):
                    mask = jnp.where(lane == lanes[c * recs + r], weights[c * recs + r], 0.0)
                    row = level + rows[c * recs + r]
                    sums = sums + mask * hist[pl.ds(row, SUB, stride=slot), :]
                return jnp.where(lane == r, jnp.sum(sums, axis=1, keepdims=True), found)
            samples[at, :] = lax.fori_loop(0, count, record, samples[at, :], unroll=unroll)

        samples[...] = jnp.zeros((TIME, recs), jnp.float32)
        lax.fori_loop(0, TIME, step, 0)

        result = pltpu.make_async_copy(
            hist.at[pl.ds((TIME + 1) * slot, block)], pressure_out, out_sem)
        result.start()
        found_at(groups - 1, 0, recs, 8)

        def g_copy(k, owner):
            return pltpu.make_async_remote_copy(
                src_ref=samples,
                dst_ref=gathered.at[pl.ds(pl.multiple_of(owner * TIME, SUB), TIME)],
                send_sem=gsend_sem.at[k],
                recv_sem=grecv_sem.at[k],
                device_id=device((me + k) % n_dev),
                device_id_type=MESH,
            )

        def push(k, carry):
            g_copy(k, me).start()
            return carry
        lax.fori_loop(1, n_dev, push, 0)
        gathered[pl.ds(pl.multiple_of(me * TIME, SUB), TIME), :] = samples[...]

        wanted = jnp.broadcast_to(order[0:1, :], (recs, recs))
        receiver = lax.broadcasted_iota(jnp.int32, (recs, recs), 0)

        def mark(d, carry):
            hit = receiver + d * recs == wanted
            onehot[pl.ds(pl.multiple_of(d * recs, recs), recs), :] = jnp.where(
                hit, 1.0, 0.0).astype(jnp.bfloat16)
            return carry
        lax.fori_loop(0, n_dev, mark, 0)

        def arrive(k, carry):
            g_copy(k, me).wait_send()
            g_copy(k, (me + n_dev - k) % n_dev).wait_recv()
            return carry
        lax.fori_loop(1, n_dev, arrive, 0)

        def reorder(d, total):
            value = gathered[pl.ds(pl.multiple_of(d * TIME, SUB), TIME), :]
            high = value.astype(jnp.bfloat16).astype(jnp.float32)
            rest = value - high
            mid = rest.astype(jnp.bfloat16).astype(jnp.float32)
            spare = jnp.zeros((-3 * TIME % 16, recs), jnp.float32)
            parts = [high, mid, rest - mid] + ([spare] if spare.shape[0] else [])
            stacked = jnp.concatenate(parts, axis=0).astype(jnp.bfloat16)
            pick = onehot[pl.ds(pl.multiple_of(d * recs, recs), recs), :]
            return total + jnp.dot(stacked, pick, preferred_element_type=jnp.float32)
        height = 3 * TIME + (-3 * TIME % 16)
        total = lax.fori_loop(
            0, n_dev, reorder, jnp.zeros((height, recs), jnp.float32), unroll=4)
        traces[...] = (total[0:TIME] + total[TIME:2 * TIME]) + total[2 * TIME:3 * TIME]
        result.wait()

    f32 = jnp.float32
    any_spec = pl.BlockSpec(memory_space=pl.ANY)
    smem = pl.BlockSpec(memory_space=pltpu.SMEM)
    return pl.pallas_call(
        kernel,
        out_shape=(
            jax.ShapeDtypeStruct((TIME, recs), f32),
            jax.ShapeDtypeStruct((block, LANE), f32),
        ),
        in_specs=[any_spec] * 6 + [smem] * 4 + [pl.BlockSpec(memory_space=pltpu.VMEM)],
        out_specs=(pl.BlockSpec(memory_space=pltpu.VMEM), any_spec),
        scratch_shapes=[
            pltpu.VMEM((slots * slot, LANE), f32),
            pltpu.VMEM((slots * 2 * plane, LANE), f32),
            pltpu.VMEM((MECH * block, LANE), f32),
            pltpu.VMEM((block, LANE), f32),
            pltpu.VMEM((block, LANE), f32),
            pltpu.VMEM((block, LANE), jnp.int32),
            pltpu.VMEM((block, LANE), f32),
            pltpu.VMEM((slots, 2, cz, xt, LANE), f32),
            pltpu.VMEM((slots, 2, cz, xt, LANE), f32),
            pltpu.VMEM((TIME, recs), f32),
            pltpu.VMEM((n_dev * TIME, recs), f32),
            pltpu.VMEM((n_dev * recs, recs), jnp.bfloat16),
            pltpu.SemaphoreType.DMA((6,)),
            pltpu.SemaphoreType.DMA((2, 2, yt)),
            pltpu.SemaphoreType.DMA((2, 2, yt)),
            pltpu.SemaphoreType.DMA((2, 2, 2)),
            pltpu.SemaphoreType.DMA((2, 2, 2)),
            pltpu.SemaphoreType.DMA((n_dev,)),
            pltpu.SemaphoreType.DMA((n_dev,)),
            pltpu.SemaphoreType.DMA,
        ],
        compiler_params=pltpu.CompilerParams(
            collective_id=0, has_side_effects=True, vmem_limit_bytes=60 * 1024 * 1024,
        ),
    )


def solution(mesh):
    n_gz, n_gy = mesh.shape["gz"], mesh.shape["gy"]

    def on_device(
        pressure, previous, memory, courant, quality, sponge, relax_time,
        receiver_cell, receiver_weight, output_order,
    ):
        cz, cy, nx = pressure.shape
        corners, recs = receiver_cell.shape
        x = receiver_cell % nx
        y = (receiver_cell // nx) % cy
        z = receiver_cell // (nx * cy)
        rows = ((z * (cy // SUB) + y // SUB) * (nx // LANE) + x // LANE) * SUB + y % SUB
        run = make_kernel(cz, cy, nx, n_gz, n_gy, corners, recs)
        traces, out = run(
            to_rows(pressure), to_rows(previous), to_rows(memory), to_rows(courant),
            to_rows(quality), to_rows(sponge), relax_time,
            rows.reshape(-1), (x % LANE).reshape(-1), receiver_weight.reshape(-1),
            output_order[None, :],
        )
        return traces, from_rows(out, (cz, cy, nx))

    in_specs = (
        P(("shots", "gz"), "gy", None),
        P(("shots", "gz"), "gy", None),
        P(None, ("shots", "gz"), "gy", None),
        P("gz", "gy", None),
        P("gz", "gy", None),
        P("gz", "gy", None),
        P(),
        P(None, ("gz", "gy")),
        P(None, ("gz", "gy")),
        P(("gz", "gy")),
    )
    out_specs = (P("shots", ("gz", "gy")), P(("shots", "gz"), "gy", None))
    return jax.shard_map(
        on_device, mesh=mesh, in_specs=in_specs, out_specs=out_specs, check_vma=False
    )
```
